32 devices in a mesh: snap: 2 (over y), row: 8 (over z, x), col: 2 (over core).
Axes of the slice: x: 2, y: 2, z: 4, core: 2. Of those that a mesh axis runs over, the one named last changes fastest.
Arguments:
- density: bfloat16 [8192, 1024], P(('snap', 'row'), 'col'), parts along dimension 0, may hold values from -0.5 to 2
- pattern: int32 [256, 32], P(('snap', 'row'), 'col'), parts along dimension 0, may hold values 0 or 1
- filter_mask: int32 [256, 32], P(('snap', 'row')), parts along dimension 0, may hold values 0 or 1
Outputs:
- purified: bfloat16 [8192, 1024], P(('snap', 'row'), 'col'), parts along dimension 0
- traces: float32 [4], P('snap'), parts along dimension 0
The draws below stay inside these ranges and needn't reach their ends.
There are 2 independent parts, one for each index of `snap`. The reference program is written for one: setup_inputs(seed, part) draws one part's arguments, and reference() takes and returns one part's arrays. A program takes and returns all parts, laid end to end along the dimension named above; each array names one. Nothing has to cross between parts.
All inputs are finite; a program needn't handle non-finite values. No bound on the sum of `pattern` or of `filter_mask` on one device may be relied on, other than what follows from the above.
Results may differ from the reference program's by a relative error of at most 0.006.
Values may be sent and summed in bfloat16 or wider, within the bound.
A program may use at most 64 MiB of HBM per device.

```python
import jax
import jax.numpy as jnp
from jax import lax

BLK = 32
S = 32
H = 16
NB = 128
ORDER = 4096


def draw_density(key, part):
    keys = jax.random.split(jax.random.fold_in(key, 11), 2)
    width = S * BLK
    sigma = 0.9 / width ** 0.5
    row_index = jnp.arange(ORDER, dtype=jnp.int32)
    offdiag = jnp.clip(jax.random.normal(keys[0], (ORDER, width), jnp.float32), -4.5, 4.5) * sigma
    rising = 0.3 + 0.6 * row_index.astype(jnp.float32) / ORDER
    occupied = jax.random.uniform(keys[1], (ORDER,), jnp.float32, 0.5, 1.5) * rising
    column_index = jnp.arange(width, dtype=jnp.int32)
    on_diagonal = column_index[None, :] == (H * BLK + row_index % BLK)[:, None]
    values = offdiag + jnp.where(on_diagonal, occupied[:, None], 0.0)
    return values.astype(jnp.bfloat16)


def place_ends(drawn, stream_key, smallest, top_value):
    longest = drawn.shape.index(max(drawn.shape))
    spots = []
    for shift in (0, 1):
        where = [jax.random.randint(jax.random.fold_in(stream_key, axis), (), 0, length) for axis, length in enumerate(drawn.shape)]
        where[longest] = (where[longest] + shift) % drawn.shape[longest]
        spots.append(tuple(where))
    return drawn.at[spots[0]].set(smallest).at[spots[1]].set(top_value)


def setup_inputs(seed: int = 0, part: int = 0) -> dict:
    streams_of = jax.random.split(jax.random.key(seed), 4)
    part_splits = jax.random.split(jax.random.fold_in(streams_of[3], part), 4)
    return {
        "density": draw_density(jax.random.fold_in(jax.random.fold_in(streams_of[3], part), 71), part),
        "pattern": place_ends((jax.random.randint(part_splits[1], (NB, S), 0, 4) < 3).astype(jnp.int32), jax.random.fold_in(part_splits[1], 1), 0, 1),
        "filter_mask": place_ends((jax.random.randint(part_splits[2], (NB, S), 0, 8) < 7).astype(jnp.int32), jax.random.fold_in(part_splits[2], 1), 0, 1),
    }


def valid_slots(row_total, slot_count, half_band):
    row_index = jnp.arange(row_total, dtype=jnp.int32)
    slot_index = jnp.arange(slot_count, dtype=jnp.int32)
    column_index = row_index[:, None] + slot_index[None, :] - half_band
    return ((column_index >= 0) & (column_index < row_total)).astype(jnp.int32)


def expand_mask(values, keep_mask):
    block_rows = keep_mask.shape[0]
    slot_count = keep_mask.shape[1]
    blocks = values.reshape(block_rows, BLK, slot_count, BLK)
    blocks = blocks * keep_mask.astype(values.dtype)[:, None, :, None]
    return blocks.reshape(block_rows * BLK, slot_count * BLK)


def shift_slots(segment, moved):
    height = segment.shape[0]
    if moved > 0:
        return jnp.concatenate([jnp.zeros((height, moved * BLK), segment.dtype), segment[:, : segment.shape[1] - moved * BLK]], 1)
    if moved < 0:
        return jnp.concatenate([segment[:, -moved * BLK:], jnp.zeros((height, -moved * BLK), segment.dtype)], 1)
    return segment


def band_product(left, right):
    group_rows = 8 if NB % 8 == 0 else 2
    extended = jnp.pad(right, ((H * BLK, H * BLK), (0, 0)))

    def one_group(group):
        first = group * group_rows
        stacked = []
        for offset in range(S):
            segment = lax.dynamic_slice_in_dim(extended, (first + offset) * BLK, group_rows * BLK, 0)
            segment = shift_slots(segment, offset - H)
            stacked.append(segment.reshape(group_rows, BLK, S * BLK))
        gathered = jnp.stack(stacked, 1).reshape(group_rows, S * BLK, S * BLK).astype(jnp.float32)
        left_rows = lax.dynamic_slice_in_dim(left, first * BLK, group_rows * BLK, 0)
        left_rows = left_rows.reshape(group_rows, BLK, S * BLK).astype(jnp.float32)
        result = jnp.einsum("gak,gkn->gan", left_rows, gathered)
        return result.reshape(group_rows * BLK, S * BLK)

    result = lax.map(one_group, jnp.arange(NB // group_rows, dtype=jnp.int32))
    return result.reshape(NB * BLK, S * BLK)


def diagonal_sum(values):
    blocks = values.reshape(NB, BLK, S, BLK)[:, :, H, :]
    return jnp.sum(jnp.diagonal(blocks, axis1=1, axis2=2).astype(jnp.float32))


def reference(density, pattern, filter_mask):
    valid = valid_slots(NB, S, H)
    kept = expand_mask(density, pattern * valid)
    square = band_product(kept, kept)
    keep_filter = filter_mask * valid
    squared = expand_mask(square, keep_filter).astype(jnp.bfloat16)
    cube = band_product(squared, kept)
    purified = (3.0 * squared.astype(jnp.float32) - 2.0 * expand_mask(cube, keep_filter)).astype(jnp.bfloat16)
    traces = jnp.stack([diagonal_sum(kept), diagonal_sum(squared)]) / ORDER
    return purified, traces
```

```python
import functools

import jax
import jax.numpy as jnp
from jax import lax
from jax.experimental import pallas as pl
from jax.experimental.pallas import tpu as pltpu
from jax.sharding import PartitionSpec as P

BLK = 32
LANE = 128
CHUNKS = 8
MESH = pl.DeviceIdType.MESH


def expander(width):
    row = lax.broadcasted_iota(jnp.int32, (LANE, width), 0)
    col = lax.broadcasted_iota(jnp.int32, (LANE, width), 1)
    return (col // BLK == row).astype(jnp.bfloat16)


def lanes_padded(value):
    short = LANE - value.shape[1]
    return jnp.concatenate([value, jnp.zeros((value.shape[0], short), value.dtype)], 1)


def valid_slots(first_row, rows, first_slot, half, total):
    row = lax.broadcasted_iota(jnp.int32, (rows, LANE), 0) + first_row
    slot = lax.broadcasted_iota(jnp.int32, (rows, LANE), 1) + first_slot
    column = row + slot - half
    return ((column >= 0) & (column < total)).astype(jnp.float32)


def kernel(
    row_size,
    density,
    pattern,
    filter_mask,
    out,
    traces,
    kept,
    near,
    right,
    squared,
    keep_filter,
    result,
    part,
    parts,
    send_sem,
    sib_sem,
    p_sem,
    psib_sem,
    q_sem,
    qsib_sem,
    tsend_sem,
    trecv_sem,
):
    rows, width = density.shape
    half = width // BLK
    block_rows = rows // BLK
    chunk = rows // CHUNKS
    snap = lax.axis_index("snap")
    me = lax.axis_index("row")
    core = lax.axis_index("col")
    odd = lax.rem(me, 2)
    partner = me + 1 - 2 * odd
    onward = me + 2 - 4 * odd
    origin = me - 2 + 4 * odd
    has_onward = (onward >= 0) & (onward < row_size)
    has_origin = (origin >= 0) & (origin < row_size)
    p_side = 1 - odd
    q_side = odd
    other = 1 - core
    total = row_size * block_rows

    barrier = pltpu.get_barrier_semaphore()

    def greet(step, _):
        peer = lax.rem(me + step, row_size)
        pl.semaphore_signal(barrier, inc=1, device_id=(snap, peer, core), device_id_type=MESH)
        return 0

    pl.semaphore_signal(barrier, inc=1, device_id=(snap, me, other), device_id_type=MESH)
    lax.fori_loop(1, row_size, greet, 0)

    first_slot = core * half
    keep = lanes_padded(pattern[...]).astype(jnp.float32)
    keep = keep * valid_slots(me * block_rows, block_rows, first_slot, half, total)
    spread = jnp.dot(keep.astype(jnp.bfloat16), expander(width), preferred_element_type=jnp.float32)
    for m in range(block_rows):
        at = pl.ds(m * BLK, BLK)
        kept[core, at, :] = (
            density[at, :].astype(jnp.float32) * spread[m : m + 1, :]
        ).astype(jnp.bfloat16)
    keep = lanes_padded(filter_mask[...]).astype(jnp.float32)
    keep = keep * valid_slots(me * block_rows, block_rows, 0, half, total)
    keep = pltpu.roll(keep, 0, 1, stride=1, stride_axis=0)
    keep_filter[...] = jnp.dot(
        keep.astype(jnp.bfloat16), expander(3 * width), preferred_element_type=jnp.float32
    )
    right[...] = jnp.zeros_like(right)

    pl.semaphore_wait(barrier, row_size)

    def block(k):
        return pl.ds(k * chunk, chunk)

    def to_partner(k):
        return pltpu.make_async_remote_copy(
            src_ref=kept.at[core, block(k), :],
            dst_ref=near.at[odd, core, block(k), :],
            send_sem=send_sem.at[0, k],
            recv_sem=p_sem.at[k],
            device_id=(snap, partner, core),
            device_id_type=MESH,
        )

    def from_partner(k):
        return pltpu.make_async_remote_copy(
            src_ref=kept.at[core, block(k), :],
            dst_ref=near.at[p_side, core, block(k), :],
            send_sem=send_sem.at[0, k],
            recv_sem=p_sem.at[k],
            device_id=(snap, partner, core),
            device_id_type=MESH,
        )

    def to_onward(k):
        return pltpu.make_async_remote_copy(
            src_ref=near.at[p_side, core, block(k), :],
            dst_ref=near.at[q_side, core, block(k), :],
            send_sem=send_sem.at[1, k],
            recv_sem=q_sem.at[k],
            device_id=(snap, onward, core),
            device_id_type=MESH,
        )

    def from_origin(k):
        return pltpu.make_async_remote_copy(
            src_ref=near.at[p_side, core, block(k), :],
            dst_ref=near.at[q_side, core, block(k), :],
            send_sem=send_sem.at[1, k],
            recv_sem=q_sem.at[k],
            device_id=(snap, origin, core),
            device_id_type=MESH,
        )

    def across(side, half_at, k, sent, received):
        return pltpu.make_async_remote_copy(
            src_ref=near.at[side, half_at, block(k), :],
            dst_ref=near.at[side, half_at, block(k), :],
            send_sem=sent,
            recv_sem=received,
            device_id=(snap, me, other),
            device_id_type=MESH,
        )

    own = pltpu.make_async_remote_copy(
        src_ref=kept.at[core],
        dst_ref=kept.at[core],
        send_sem=send_sem.at[4, 0],
        recv_sem=sib_sem,
        device_id=(snap, me, other),
        device_id_type=MESH,
    )
    own_in = pltpu.make_async_remote_copy(
        src_ref=kept.at[other],
        dst_ref=kept.at[other],
        send_sem=send_sem.at[4, 0],
        recv_sem=sib_sem,
        device_id=(snap, me, other),
        device_id_type=MESH,
    )
    own.start()
    for k in range(CHUNKS):
        to_partner(k).start()
    own_in.wait_recv()

    def skew(first, second, m, row_base, lane_base):
        at = pl.ds(m * BLK, BLK)
        band = jnp.concatenate(
            [first[at, :], second[at, :], jnp.zeros((BLK, LANE), jnp.bfloat16)], 1
        )
        turn = (m * BLK) % LANE
        if turn:
            band = pltpu.roll(band.astype(jnp.float32), turn, 1).astype(jnp.bfloat16)
        start = lane_base + m * BLK - turn
        low = max(0, -start)
        high = min(band.shape[1], 3 * width - start)
        right[pl.ds(row_base + m * BLK, BLK), pl.ds(start + low, high - low)] = band[:, low:high]

    for m in range(block_rows):
        skew(kept.at[0], kept.at[1], m, rows, 0)

    @pl.when(jnp.logical_not(has_origin))
    def _():
        near[q_side] = jnp.zeros(near.shape[1:], near.dtype)

    for k in range(CHUNKS):
        from_partner(k).wait_recv()
        across(p_side, core, k, send_sem.at[2, k], psib_sem.at[k]).start()

        @pl.when(has_onward)
        def _():
            to_onward(k).start()

    for k in range(CHUNKS):

        @pl.when(has_origin)
        def _():
            from_origin(k).wait_recv()
            across(q_side, core, k, send_sem.at[3, k], qsib_sem.at[k]).start()

        across(p_side, other, k, send_sem.at[2, k], psib_sem.at[k]).wait_recv()

    @pl.when(has_origin)
    def _():
        for k in range(CHUNKS):
            across(q_side, other, k, send_sem.at[3, k], qsib_sem.at[k]).wait_recv()

    for m in range(block_rows):
        skew(near.at[0, 0], near.at[0, 1], m, 0, -width)
    for m in range(block_rows):
        skew(near.at[1, 0], near.at[1, 1], m, 2 * rows, width)

    step = width // 2
    for n in range(6):
        at = pl.ds(n * step, step)
        deep = pl.ds(rows if n >= 4 else 0, (3 if n in (2, 3) else 2) * rows)
        tile = jnp.dot(
            right[pl.ds(rows, rows), deep], right[deep, at], preferred_element_type=jnp.float32
        )
        for m in range(block_rows):
            squared[pl.ds(m * BLK, BLK), at] = (
                tile[m * BLK : (m + 1) * BLK] * keep_filter[m : m + 1, at]
            ).astype(jnp.bfloat16)

    lane = lax.broadcasted_iota(jnp.int32, (LANE, LANE), 1)
    diagonal = lane == lax.broadcasted_iota(jnp.int32, (LANE, LANE), 0)
    kept_sum = jnp.zeros((LANE, LANE), jnp.float32)
    squared_sum = jnp.zeros((LANE, LANE), jnp.float32)
    for b in range(rows // LANE):
        here = pl.ds(width + b * LANE, LANE)
        kept_sum += jnp.where(
            diagonal, right[pl.ds(rows + b * LANE, LANE), here].astype(jnp.float32), 0.0
        )
        squared_sum += jnp.where(
            diagonal, squared[pl.ds(b * LANE, LANE), here].astype(jnp.float32), 0.0
        )
    part[0] = jnp.sum(kept_sum.reshape(LANE // 8, 8, LANE), 0)
    part[1] = jnp.sum(squared_sum.reshape(LANE // 8, 8, LANE), 0)

    left = pl.multiple_of(core * width, LANE)
    for n in range(4):
        at = pl.ds(pl.multiple_of(left + n * step, LANE), step)
        tile = jnp.dot(squared[...], right[:, at], preferred_element_type=jnp.float32)
        for m in range(block_rows):
            rows_at = pl.ds(m * BLK, BLK)
            result[rows_at, pl.ds(n * step, step)] = (
                3.0 * squared[rows_at, at].astype(jnp.float32)
                - 2.0 * (tile[m * BLK : (m + 1) * BLK] * keep_filter[m : m + 1, at])
            )
        if n == 0:

            def share(step_to, _):
                peer = lax.rem(me + step_to, row_size)
                pltpu.make_async_remote_copy(
                    src_ref=part,
                    dst_ref=parts.at[step_to],
                    send_sem=tsend_sem.at[step_to],
                    recv_sem=trecv_sem.at[step_to],
                    device_id=(snap, peer, core),
                    device_id_type=MESH,
                ).start()
                return 0

            lax.fori_loop(1, row_size, share, 0)

    for m in range(block_rows):
        turn = (m * BLK) % LANE
        start = m * BLK - turn
        band = result[pl.ds(m * BLK, BLK), pl.ds(start, width + (LANE if turn else 0))]
        if turn:
            band = pltpu.roll(band, band.shape[1] - turn, 1)
        out[pl.ds(m * BLK, BLK), :] = band[:, :width].astype(jnp.bfloat16)

    def gather(step_to, sums):
        peer = lax.rem(me + row_size - step_to, row_size)
        pltpu.make_async_remote_copy(
            src_ref=part,
            dst_ref=parts.at[step_to],
            send_sem=tsend_sem.at[step_to],
            recv_sem=trecv_sem.at[step_to],
            device_id=(snap, peer, core),
            device_id_type=MESH,
        ).wait()
        return (sums[0] + parts[step_to, 0], sums[1] + parts[step_to, 1])

    sums = lax.fori_loop(1, row_size, gather, (part[0], part[1]))
    traces[0] = jnp.sum(sums[0]) / (total * BLK)
    traces[1] = jnp.sum(sums[1]) / (total * BLK)

    own.wait_send()
    for k in range(CHUNKS):
        to_partner(k).wait_send()
        across(p_side, core, k, send_sem.at[2, k], psib_sem.at[k]).wait_send()

        @pl.when(has_onward)
        def _():
            to_onward(k).wait_send()

        @pl.when(has_origin)
        def _():
            across(q_side, core, k, send_sem.at[3, k], qsib_sem.at[k]).wait_send()


def solution(mesh):
    row_size = mesh.shape["row"]

    def per_device(density, pattern, filter_mask):
        rows, width = density.shape
        block_rows = rows // BLK
        return pl.pallas_call(
            functools.partial(kernel, row_size),
            out_shape=(
                jax.ShapeDtypeStruct((rows, width), jnp.bfloat16),
                jax.ShapeDtypeStruct((2,), jnp.float32),
            ),
            in_specs=[pl.BlockSpec(memory_space=pltpu.VMEM)] * 3,
            out_specs=(
                pl.BlockSpec(memory_space=pltpu.VMEM),
                pl.BlockSpec(memory_space=pltpu.SMEM),
            ),
            scratch_shapes=[
                pltpu.VMEM((2, rows, width), jnp.bfloat16),
                pltpu.VMEM((2, 2, rows, width), jnp.bfloat16),
                pltpu.VMEM((3 * rows, 3 * width), jnp.bfloat16),
                pltpu.VMEM((rows, 3 * width), jnp.bfloat16),
                pltpu.VMEM((block_rows, 3 * width), jnp.float32),
                pltpu.VMEM((rows, 2 * width), jnp.float32),
                pltpu.VMEM((2, 8, LANE), jnp.float32),
                pltpu.VMEM((row_size, 2, 8, LANE), jnp.float32),
                pltpu.SemaphoreType.DMA((5, CHUNKS)),
                pltpu.SemaphoreType.DMA,
                pltpu.SemaphoreType.DMA((CHUNKS,)),
                pltpu.SemaphoreType.DMA((CHUNKS,)),
                pltpu.SemaphoreType.DMA((CHUNKS,)),
                pltpu.SemaphoreType.DMA((CHUNKS,)),
                pltpu.SemaphoreType.DMA((row_size,)),
                pltpu.SemaphoreType.DMA((row_size,)),
            ],
            compiler_params=pltpu.CompilerParams(
                collective_id=0, has_side_effects=True, vmem_limit_bytes=56 * 1024 * 1024
            ),
        )(density, pattern, filter_mask)

    return jax.shard_map(
        per_device,
        mesh=mesh,
        in_specs=(P(("snap", "row"), "col"), P(("snap", "row"), "col"), P(("snap", "row"), None)),
        out_specs=(P(("snap", "row"), "col"), P("snap")),
        check_vma=False,
    )
```

```python
import functools

import jax
import jax.numpy as jnp
from jax import lax
from jax.experimental import pallas as pl
from jax.experimental.pallas import tpu as pltpu
from jax.sharding import PartitionSpec as P

BLK = 32
LANE = 128
CHUNKS = 8
LAG = 3
MESH = pl.DeviceIdType.MESH


def expander(width):
    row = lax.broadcasted_iota(jnp.int32, (LANE, width), 0)
    col = lax.broadcasted_iota(jnp.int32, (LANE, width), 1)
    return (col // BLK == row).astype(jnp.bfloat16)


def lanes_padded(value):
    short = LANE - value.shape[1]
    return jnp.concatenate([value, jnp.zeros((value.shape[0], short), value.dtype)], 1)


def valid_slots(first_row, rows, first_slot, half, total):
    row = lax.broadcasted_iota(jnp.int32, (rows, LANE), 0) + first_row
    slot = lax.broadcasted_iota(jnp.int32, (rows, LANE), 1) + first_slot
    column = row + slot - half
    return ((column >= 0) & (column < total)).astype(jnp.float32)


def kernel(
    row_size,
    density_in,
    pattern_in,
    filter_in,
    out,
    traces,
    density,
    pattern,
    filter_mask,
    kept,
    near,
    right,
    total_sum,
    squared,
    keep_filter,
    result,
    part,
    parts,
    send_sem,
    sib_sem,
    p_sem,
    psib_sem,
    q_sem,
    qsib_sem,
    tsend_sem,
    trecv_sem,
    load_sem,
    round_sem,
    done_sem,
):
    rows, width = density_in.shape
    half = width // BLK
    block_rows = rows // BLK
    chunk = rows // CHUNKS
    snap = lax.axis_index("snap")
    me = lax.axis_index("row")
    core = lax.axis_index("col")
    odd = lax.rem(me, 2)
    partner = me + 1 - 2 * odd
    onward = me + 2 - 4 * odd
    origin = me - 2 + 4 * odd
    has_onward = (onward >= 0) & (onward < row_size)
    has_origin = (origin >= 0) & (origin < row_size)
    p_side = 1 - odd
    q_side = odd
    other = 1 - core
    total = row_size * block_rows

    barrier = pltpu.get_barrier_semaphore()

    def greet(row, column, semaphore):
        pl.semaphore_signal(semaphore, inc=1, device_id=(snap, row, column), device_id_type=MESH)

    greet(me, other, barrier)
    greet(partner, core, barrier)

    @pl.when(has_onward)
    def _():
        greet(onward, core, barrier)

    @pl.when(has_origin)
    def _():
        greet(origin, core, barrier)

    beside = has_onward.astype(jnp.int32) + has_origin.astype(jnp.int32)
    loads = [
        pltpu.make_async_copy(source, target, load_sem.at[i])
        for i, (source, target) in enumerate(
            ((density_in, density), (pattern_in, pattern), (filter_in, filter_mask))
        )
    ]
    for load in loads:
        load.start()
    loads[1].wait()
    first_slot = core * half
    keep = lanes_padded(pattern[...]).astype(jnp.float32)
    keep = keep * valid_slots(me * block_rows, block_rows, first_slot, half, total)
    spread = jnp.dot(keep.astype(jnp.bfloat16), expander(width), preferred_element_type=jnp.float32)
    loads[0].wait()
    for m in range(block_rows):
        at = pl.ds(m * BLK, BLK)
        kept[core, at, :] = (
            density[at, :].astype(jnp.float32) * spread[m : m + 1, :]
        ).astype(jnp.bfloat16)
    pl.semaphore_wait(barrier, 2 + beside)

    def block(k):
        return pl.ds(k * chunk, chunk)

    def to_partner(k):
        return pltpu.make_async_remote_copy(
            src_ref=kept.at[core, block(k), :],
            dst_ref=near.at[odd, core, block(k), :],
            send_sem=send_sem.at[0, k],
            recv_sem=p_sem.at[k],
            device_id=(snap, partner, core),
            device_id_type=MESH,
        )

    def from_partner(k):
        return pltpu.make_async_remote_copy(
            src_ref=kept.at[core, block(k), :],
            dst_ref=near.at[p_side, core, block(k), :],
            send_sem=send_sem.at[0, k],
            recv_sem=p_sem.at[k],
            device_id=(snap, partner, core),
            device_id_type=MESH,
        )

    def to_onward(k):
        return pltpu.make_async_remote_copy(
            src_ref=near.at[p_side, core, block(k), :],
            dst_ref=near.at[q_side, core, block(k), :],
            send_sem=send_sem.at[1, k],
            recv_sem=q_sem.at[k],
            device_id=(snap, onward, core),
            device_id_type=MESH,
        )

    def from_origin(k):
        return pltpu.make_async_remote_copy(
            src_ref=near.at[p_side, core, block(k), :],
            dst_ref=near.at[q_side, core, block(k), :],
            send_sem=send_sem.at[1, k],
            recv_sem=q_sem.at[k],
            device_id=(snap, origin, core),
            device_id_type=MESH,
        )

    def across(side, half_at, k, sent, received):
        return pltpu.make_async_remote_copy(
            src_ref=near.at[side, half_at, block(k), :],
            dst_ref=near.at[side, half_at, block(k), :],
            send_sem=sent,
            recv_sem=received,
            device_id=(snap, me, other),
            device_id_type=MESH,
        )

    own = pltpu.make_async_remote_copy(
        src_ref=kept.at[core],
        dst_ref=kept.at[core],
        send_sem=send_sem.at[4, 0],
        recv_sem=sib_sem,
        device_id=(snap, me, other),
        device_id_type=MESH,
    )
    own_in = pltpu.make_async_remote_copy(
        src_ref=kept.at[other],
        dst_ref=kept.at[other],
        send_sem=send_sem.at[4, 0],
        recv_sem=sib_sem,
        device_id=(snap, me, other),
        device_id_type=MESH,
    )
    own.start()
    for k in range(CHUNKS):
        to_partner(k).start()
    loads[2].wait()
    keep = lanes_padded(filter_mask[...]).astype(jnp.float32)
    keep = keep * valid_slots(me * block_rows, block_rows, 0, half, total)
    keep = pltpu.roll(keep, 0, 1, stride=1, stride_axis=0)
    keep_filter[...] = jnp.dot(
        keep.astype(jnp.bfloat16), expander(3 * width), preferred_element_type=jnp.float32
    )
    right[:, pl.ds(width, 3 * width)] = jnp.zeros((3 * rows, 3 * width), right.dtype)

    own_in.wait_recv()

    def skew(first, second, m, side):
        at = pl.ds(m * BLK, BLK)
        band = jnp.concatenate(
            [first[at, :], second[at, :], jnp.zeros((BLK, LANE), jnp.bfloat16)], 1
        )
        turn = (m * BLK) % LANE
        if turn:
            band = pltpu.roll(band.astype(jnp.float32), turn, 1).astype(jnp.bfloat16)
        to_row = pl.multiple_of(side * rows + m * BLK, BLK)
        to_lane = pl.multiple_of(side * width + m * BLK - turn, LANE)
        right[pl.ds(to_row, BLK), pl.ds(to_lane, 2 * width + LANE)] = band

    for m in range(block_rows):
        skew(kept.at[0], kept.at[1], m, 1)

    @pl.when(jnp.logical_not(has_origin))
    def _():
        near[q_side] = jnp.zeros(near.shape[1:], near.dtype)

    def meet(level, _):
        @pl.when(has_onward)
        def _():
            greet(onward, core, round_sem.at[level])

        @pl.when(has_origin)
        def _():
            greet(origin, core, round_sem.at[level])

        pl.semaphore_wait(round_sem.at[level], beside)
        return 0

    lax.fori_loop(1, row_size // 2, meet, 0)
    greet(partner, core, done_sem)

    step = width // 2

    def own_product(n):
        at = pl.ds(n * step, step)
        total_sum[:, at] = jnp.dot(
            right[pl.ds(rows, rows), pl.ds(2 * width, width)],
            right[pl.ds(rows, rows), pl.ds(width + n * step, step)],
            preferred_element_type=jnp.float32,
        )

    def side_product(side, part_at):
        depth = rows // 2
        from_row = pl.multiple_of(side * rows + part_at * depth, LANE)
        from_lane = pl.multiple_of((1 + side) * width + part_at * depth, LANE)
        to_lane = (side // 2) * width
        for n in range(4):
            at = pl.multiple_of(to_lane + n * step, LANE)
            total_sum[:, pl.ds(at, step)] += jnp.dot(
                right[pl.ds(rows, rows), pl.ds(from_lane, depth)],
                right[pl.ds(from_row, depth), pl.ds(pl.multiple_of(width + at, LANE), step)],
                preferred_element_type=jnp.float32,
            )

    def lay(side, k):
        for m in range(k * chunk // BLK, (k + 1) * chunk // BLK):
            skew(near.at[side, 0], near.at[side, 1], m, 2 * side)

    for k in range(CHUNKS + LAG + 1):
        if k < CHUNKS:
            from_partner(k).wait_recv()
            across(p_side, core, k, send_sem.at[2, k], psib_sem.at[k]).start()

            @pl.when(has_onward)
            def _():
                to_onward(k).start()

        if 0 <= k - LAG < CHUNKS:

            @pl.when(has_origin)
            def _():
                from_origin(k - LAG).wait_recv()
                across(q_side, core, k - LAG, send_sem.at[3, k - LAG], qsib_sem.at[k - LAG]).start()

        if k < 6:
            own_product(k)
        late = k - 1
        if 0 <= late < CHUNKS:
            across(p_side, other, late, send_sem.at[2, late], psib_sem.at[late]).wait_recv()
            lay(p_side, late)
            if late == CHUNKS - 1:
                side_product(2 * p_side, 1)
        late = k - 1 - LAG
        if 0 <= late < CHUNKS:

            @pl.when(has_origin)
            def _():
                across(q_side, other, late, send_sem.at[3, late], qsib_sem.at[late]).wait_recv()

            lay(q_side, late)
        if k == max(6, CHUNKS // 2 + 1):
            side_product(2 * p_side, 0)
        if k == max(7, CHUNKS // 2 + 1 + LAG):
            side_product(2 * q_side, 0)
    side_product(2 * q_side, 1)
    pl.semaphore_wait(done_sem, 1)

    for m in range(block_rows):
        at = pl.ds(m * BLK, BLK)
        squared[at, :] = (total_sum[at, :] * keep_filter[m : m + 1, :]).astype(jnp.bfloat16)

    lane = lax.broadcasted_iota(jnp.int32, (LANE, LANE), 1)
    diagonal = lane == lax.broadcasted_iota(jnp.int32, (LANE, LANE), 0)
    kept_sum = jnp.zeros((LANE, LANE), jnp.float32)
    squared_sum = jnp.zeros((LANE, LANE), jnp.float32)
    for b in range(rows // LANE):
        here = pl.ds(width + b * LANE, LANE)
        kept_sum += jnp.where(
            diagonal, right[pl.ds(rows + b * LANE, LANE), pl.ds(2 * width + b * LANE, LANE)].astype(jnp.float32), 0.0
        )
        squared_sum += jnp.where(
            diagonal, squared[pl.ds(b * LANE, LANE), here].astype(jnp.float32), 0.0
        )
    part[0] = jnp.sum(kept_sum.reshape(LANE // 8, 8, LANE), 0)
    part[1] = jnp.sum(squared_sum.reshape(LANE // 8, 8, LANE), 0)

    for n in range(4):
        if n < 2:
            column = width + n * step
            place = (1 - core) * width + n * step
            deep = pl.ds(0, 3 * rows)
        else:
            column = 2 * core * width + (n - 2) * step
            place = core * width + (n - 2) * step
            deep = pl.ds(pl.multiple_of(core * rows, LANE), 2 * rows)
        at = pl.ds(pl.multiple_of(column, LANE), step)
        place = pl.ds(pl.multiple_of(place, LANE), step)
        tile = jnp.dot(
            squared[:, deep],
            right[deep, pl.ds(pl.multiple_of(width + column, LANE), step)],
            preferred_element_type=jnp.float32,
        )
        for m in range(block_rows):
            rows_at = pl.ds(m * BLK, BLK)
            result[rows_at, place] = 3.0 * squared[rows_at, at].astype(jnp.float32) - 2.0 * (
                tile[m * BLK : (m + 1) * BLK] * keep_filter[pl.ds(m, 1), at]
            )
        if n == 0:

            def share(step_to, _):
                peer = lax.rem(me + step_to, row_size)
                pltpu.make_async_remote_copy(
                    src_ref=part,
                    dst_ref=parts.at[step_to],
                    send_sem=tsend_sem.at[step_to],
                    recv_sem=trecv_sem.at[step_to],
                    device_id=(snap, peer, core),
                    device_id_type=MESH,
                ).start()
                return 0

            lax.fori_loop(1, row_size, share, 0)

    for m in range(block_rows):
        turn = (m * BLK) % LANE
        start = m * BLK - turn
        band = result[pl.ds(m * BLK, BLK), pl.ds(start, width + (LANE if turn else 0))]
        if turn:
            band = pltpu.roll(band, band.shape[1] - turn, 1)
        out[pl.ds(m * BLK, BLK), :] = band[:, :width].astype(jnp.bfloat16)

    def gather(step_to, sums):
        peer = lax.rem(me + row_size - step_to, row_size)
        pltpu.make_async_remote_copy(
            src_ref=part,
            dst_ref=parts.at[step_to],
            send_sem=tsend_sem.at[step_to],
            recv_sem=trecv_sem.at[step_to],
            device_id=(snap, peer, core),
            device_id_type=MESH,
        ).wait()
        return (sums[0] + parts[step_to, 0], sums[1] + parts[step_to, 1])

    sums = lax.fori_loop(1, row_size, gather, (part[0], part[1]))
    traces[0] = jnp.sum(sums[0]) / (total * BLK)
    traces[1] = jnp.sum(sums[1]) / (total * BLK)

    own.wait_send()
    for k in range(CHUNKS):
        to_partner(k).wait_send()
        across(p_side, core, k, send_sem.at[2, k], psib_sem.at[k]).wait_send()

        @pl.when(has_onward)
        def _():
            to_onward(k).wait_send()

        @pl.when(has_origin)
        def _():
            across(q_side, core, k, send_sem.at[3, k], qsib_sem.at[k]).wait_send()


def solution(mesh):
    row_size = mesh.shape["row"]

    def per_device(density, pattern, filter_mask):
        rows, width = density.shape
        block_rows = rows // BLK
        return pl.pallas_call(
            functools.partial(kernel, row_size),
            out_shape=(
                pltpu.VMEM((rows, width), jnp.bfloat16),
                jax.ShapeDtypeStruct((2,), jnp.float32),
            ),
            in_specs=[pl.BlockSpec(memory_space=pl.ANY)] * 3,
            out_specs=(
                pl.BlockSpec(memory_space=pltpu.VMEM),
                pl.BlockSpec(memory_space=pltpu.SMEM),
            ),
            scratch_shapes=[
                pltpu.VMEM((rows, width), jnp.bfloat16),
                pltpu.VMEM(pattern.shape, jnp.int32),
                pltpu.VMEM(filter_mask.shape, jnp.int32),
                pltpu.VMEM((2, rows, width), jnp.bfloat16),
                pltpu.VMEM((2, 2, rows, width), jnp.bfloat16),
                pltpu.VMEM((3 * rows, 5 * width), jnp.bfloat16),
                pltpu.VMEM((rows, 3 * width), jnp.float32),
                pltpu.VMEM((rows, 3 * width), jnp.bfloat16),
                pltpu.VMEM((block_rows, 3 * width), jnp.float32),
                pltpu.VMEM((rows, 2 * width), jnp.float32),
                pltpu.VMEM((2, 8, LANE), jnp.float32),
                pltpu.VMEM((row_size, 2, 8, LANE), jnp.float32),
                pltpu.SemaphoreType.DMA((5, CHUNKS)),
                pltpu.SemaphoreType.DMA,
                pltpu.SemaphoreType.DMA((CHUNKS,)),
                pltpu.SemaphoreType.DMA((CHUNKS,)),
                pltpu.SemaphoreType.DMA((CHUNKS,)),
                pltpu.SemaphoreType.DMA((CHUNKS,)),
                pltpu.SemaphoreType.DMA((row_size,)),
                pltpu.SemaphoreType.DMA((row_size,)),
                pltpu.SemaphoreType.DMA((3,)),
                pltpu.SemaphoreType.REGULAR((max(row_size // 2, 1),)),
                pltpu.SemaphoreType.REGULAR,
            ],
            compiler_params=pltpu.CompilerParams(
                collective_id=0, has_side_effects=True, vmem_limit_bytes=56 * 1024 * 1024
            ),
        )(density, pattern, filter_mask)

    return jax.shard_map(
        per_device,
        mesh=mesh,
        in_specs=(P(("snap", "row"), "col"), P(("snap", "row"), "col"), P(("snap", "row"), None)),
        out_specs=(P(("snap", "row"), "col"), P("snap")),
        check_vma=False,
    )
```

```python
import functools

import jax
import jax.numpy as jnp
from jax import lax
from jax.experimental import pallas as pl
from jax.experimental.pallas import tpu as pltpu
from jax.sharding import PartitionSpec as P

BLK = 32
LANE = 128
CHUNKS = 8
LAG = 3
MESH = pl.DeviceIdType.MESH


def expander(width):
    row = lax.broadcasted_iota(jnp.int32, (LANE, width), 0)
    col = lax.broadcasted_iota(jnp.int32, (LANE, width), 1)
    return (col // BLK == row).astype(jnp.bfloat16)


def lanes_padded(value):
    short = LANE - value.shape[1]
    return jnp.concatenate([value, jnp.zeros((value.shape[0], short), value.dtype)], 1)


def valid_slots(first_row, rows, first_slot, half, total):
    row = lax.broadcasted_iota(jnp.int32, (rows, LANE), 0) + first_row
    slot = lax.broadcasted_iota(jnp.int32, (rows, LANE), 1) + first_slot
    column = row + slot - half
    return ((column >= 0) & (column < total)).astype(jnp.float32)


def kernel(
    row_size,
    density_in,
    pattern_in,
    filter_in,
    out,
    traces,
    density,
    pattern,
    filter_mask,
    kept,
    near,
    right,
    total_sum,
    squared,
    keep_filter,
    result,
    part,
    parts,
    send_sem,
    sib_sem,
    p_sem,
    psib_sem,
    q_sem,
    qsib_sem,
    tsend_sem,
    trecv_sem,
    load_sem,
    round_sem,
    done_sem,
):
    rows, width = density_in.shape
    half = width // BLK
    block_rows = rows // BLK
    chunk = rows // CHUNKS
    snap = lax.axis_index("snap")
    me = lax.axis_index("row")
    core = lax.axis_index("col")
    odd = lax.rem(me, 2)
    partner = me + 1 - 2 * odd
    onward = me + 2 - 4 * odd
    origin = me - 2 + 4 * odd
    has_onward = (onward >= 0) & (onward < row_size)
    has_origin = (origin >= 0) & (origin < row_size)
    p_side = 1 - odd
    q_side = odd
    other = 1 - core
    total = row_size * block_rows

    barrier = pltpu.get_barrier_semaphore()

    def greet(row, column, semaphore):
        pl.semaphore_signal(semaphore, inc=1, device_id=(snap, row, column), device_id_type=MESH)

    greet(me, other, barrier)
    greet(partner, core, barrier)

    @pl.when(has_onward)
    def _():
        greet(onward, core, barrier)

    @pl.when(has_origin)
    def _():
        greet(origin, core, barrier)

    beside = has_onward.astype(jnp.int32) + has_origin.astype(jnp.int32)
    loads = [
        pltpu.make_async_copy(source, target, load_sem.at[i])
        for i, (source, target) in enumerate(
            ((density_in, density), (pattern_in, pattern), (filter_in, filter_mask))
        )
    ]
    for load in loads:
        load.start()
    loads[1].wait()
    first_slot = core * half
    keep = lanes_padded(pattern[...]).astype(jnp.float32)
    keep = keep * valid_slots(me * block_rows, block_rows, first_slot, half, total)
    spread = jnp.dot(keep.astype(jnp.bfloat16), expander(width), preferred_element_type=jnp.float32)
    loads[0].wait()
    for m in range(block_rows):
        at = pl.ds(m * BLK, BLK)
        kept[core, at, :] = (
            density[at, :].astype(jnp.float32) * spread[m : m + 1, :]
        ).astype(jnp.bfloat16)
    pl.semaphore_wait(barrier, 2 + beside)

    def block(k):
        return pl.ds(k * chunk, chunk)

    def lanes(k, short):
        above = k * chunk // LANE * LANE
        if short == 0:
            return pl.ds(0, width)
        if short == 1:
            return pl.ds(0, width - above)
        return pl.ds(rows - above - LANE, above + LANE)

    def either(exists, act):
        @pl.when(exists & (core == odd) & (odd == 1))
        def _():
            act(1)

        @pl.when(exists & (core == odd) & (odd == 0))
        def _():
            act(2)

        @pl.when(exists & (core != odd))
        def _():
            act(0)

    def to_partner(k):
        return pltpu.make_async_remote_copy(
            src_ref=kept.at[core, block(k), :],
            dst_ref=near.at[odd, core, block(k), :],
            send_sem=send_sem.at[0, k],
            recv_sem=p_sem.at[k],
            device_id=(snap, partner, core),
            device_id_type=MESH,
        )

    def from_partner(k):
        return pltpu.make_async_remote_copy(
            src_ref=kept.at[core, block(k), :],
            dst_ref=near.at[p_side, core, block(k), :],
            send_sem=send_sem.at[0, k],
            recv_sem=p_sem.at[k],
            device_id=(snap, partner, core),
            device_id_type=MESH,
        )

    def to_onward(k, short):
        return pltpu.make_async_remote_copy(
            src_ref=near.at[p_side, core, block(k), lanes(k, short)],
            dst_ref=near.at[q_side, core, block(k), lanes(k, short)],
            send_sem=send_sem.at[1, k],
            recv_sem=q_sem.at[k],
            device_id=(snap, onward, core),
            device_id_type=MESH,
        )

    def from_origin(k, short):
        return pltpu.make_async_remote_copy(
            src_ref=near.at[p_side, core, block(k), lanes(k, short)],
            dst_ref=near.at[q_side, core, block(k), lanes(k, short)],
            send_sem=send_sem.at[1, k],
            recv_sem=q_sem.at[k],
            device_id=(snap, origin, core),
            device_id_type=MESH,
        )

    def across(side, half_at, k, sent, received):
        return pltpu.make_async_remote_copy(
            src_ref=near.at[side, half_at, block(k), :],
            dst_ref=near.at[side, half_at, block(k), :],
            send_sem=sent,
            recv_sem=received,
            device_id=(snap, me, other),
            device_id_type=MESH,
        )

    own = pltpu.make_async_remote_copy(
        src_ref=kept.at[core],
        dst_ref=kept.at[core],
        send_sem=send_sem.at[4, 0],
        recv_sem=sib_sem,
        device_id=(snap, me, other),
        device_id_type=MESH,
    )
    own_in = pltpu.make_async_remote_copy(
        src_ref=kept.at[other],
        dst_ref=kept.at[other],
        send_sem=send_sem.at[4, 0],
        recv_sem=sib_sem,
        device_id=(snap, me, other),
        device_id_type=MESH,
    )
    own.start()
    for k in range(CHUNKS):
        to_partner(k).start()
    loads[2].wait()
    keep = lanes_padded(filter_mask[...]).astype(jnp.float32)
    keep = keep * valid_slots(me * block_rows, block_rows, 0, half, total)
    keep = pltpu.roll(keep, 0, 1, stride=1, stride_axis=0)
    keep_filter[...] = jnp.dot(
        keep.astype(jnp.bfloat16), expander(3 * width), preferred_element_type=jnp.float32
    )
    right[:, pl.ds(width, 3 * width)] = jnp.zeros((3 * rows, 3 * width), right.dtype)

    own_in.wait_recv()

    def skew(first, second, m, side):
        at = pl.ds(m * BLK, BLK)
        band = jnp.concatenate(
            [first[at, :], second[at, :], jnp.zeros((BLK, LANE), jnp.bfloat16)], 1
        )
        turn = (m * BLK) % LANE
        if turn:
            band = pltpu.roll(band.astype(jnp.float32), turn, 1).astype(jnp.bfloat16)
        to_row = pl.multiple_of(side * rows + m * BLK, BLK)
        to_lane = pl.multiple_of(side * width + m * BLK - turn, LANE)
        right[pl.ds(to_row, BLK), pl.ds(to_lane, 2 * width + LANE)] = band

    for m in range(block_rows):
        skew(kept.at[0], kept.at[1], m, 1)

    @pl.when(jnp.logical_not(has_origin))
    def _():
        near[q_side] = jnp.zeros(near.shape[1:], near.dtype)

    levels = row_size // 2

    def meet(level):
        @pl.when(has_onward)
        def _():
            greet(onward, core, round_sem.at[level])

        @pl.when(has_origin)
        def _():
            greet(origin, core, round_sem.at[level])

    def met(level):
        pl.semaphore_wait(round_sem.at[level], beside)

    def meet_again(level, _):
        meet(level)
        met(level)
        return 0

    step = width // 2

    def own_product(n):
        at = pl.ds(n * step, step)
        total_sum[:, at] = jnp.dot(
            right[pl.ds(rows, rows), pl.ds(2 * width, width)],
            right[pl.ds(rows, rows), pl.ds(width + n * step, step)],
            preferred_element_type=jnp.float32,
        )

    def side_product(side, part_at):
        depth = rows // 2
        from_row = pl.multiple_of(side * rows + part_at * depth, LANE)
        from_lane = pl.multiple_of((1 + side) * width + part_at * depth, LANE)
        to_lane = (side // 2) * width
        for n in range(4):
            at = pl.multiple_of(to_lane + n * step, LANE)
            total_sum[:, pl.ds(at, step)] += jnp.dot(
                right[pl.ds(rows, rows), pl.ds(from_lane, depth)],
                right[pl.ds(from_row, depth), pl.ds(pl.multiple_of(width + at, LANE), step)],
                preferred_element_type=jnp.float32,
            )

    def lay(side, k):
        for m in range(k * chunk // BLK, (k + 1) * chunk // BLK):
            skew(near.at[side, 0], near.at[side, 1], m, 2 * side)

    for k in range(CHUNKS + LAG + 1):
        if k < CHUNKS:
            from_partner(k).wait_recv()
            across(p_side, core, k, send_sem.at[2, k], psib_sem.at[k]).start()

            either(has_onward, lambda short: to_onward(k, short).start())

        if 0 <= k - LAG < CHUNKS:

            either(has_origin, lambda short: from_origin(k - LAG, short).wait_recv())

            @pl.when(has_origin)
            def _():
                across(q_side, core, k - LAG, send_sem.at[3, k - LAG], qsib_sem.at[k - LAG]).start()

        if 1 <= k - 1 < levels:
            met(k - 1)
        if 1 <= k < levels:
            meet(k)
        if k < 6:
            own_product(k)
        late = k - 1
        if 0 <= late < CHUNKS:
            across(p_side, other, late, send_sem.at[2, late], psib_sem.at[late]).wait_recv()
            lay(p_side, late)
            if late == CHUNKS - 1:
                side_product(2 * p_side, 1)
        late = k - 1 - LAG
        if 0 <= late < CHUNKS:

            @pl.when(has_origin)
            def _():
                across(q_side, other, late, send_sem.at[3, late], qsib_sem.at[late]).wait_recv()

            lay(q_side, late)
        if k == max(6, CHUNKS // 2 + 1):
            side_product(2 * p_side, 0)
        if k == max(7, CHUNKS // 2 + 1 + LAG):
            side_product(2 * q_side, 0)
        if k == min(CHUNKS, levels):
            if k < levels:
                met(k)
                lax.fori_loop(k + 1, levels, meet_again, 0)
            greet(partner, core, done_sem)
    side_product(2 * q_side, 1)
    pl.semaphore_wait(done_sem, 1)

    lane = lax.broadcasted_iota(jnp.int32, (LANE, LANE), 1)
    diagonal = lane == lax.broadcasted_iota(jnp.int32, (LANE, LANE), 0)
    kept_sum = jnp.zeros((LANE, LANE), jnp.float32)
    squared_sum = jnp.zeros((LANE, LANE), jnp.float32)
    for b in range(rows // LANE):
        here = pl.ds(width + b * LANE, LANE)
        kept_sum += jnp.where(
            diagonal, right[pl.ds(rows + b * LANE, LANE), pl.ds(2 * width + b * LANE, LANE)].astype(jnp.float32), 0.0
        )
        blocks = []
        for m in range(b * LANE // BLK, (b + 1) * LANE // BLK):
            blocks.append(total_sum[pl.ds(m * BLK, BLK), here] * keep_filter[pl.ds(m, 1), here])
        rounded = jnp.concatenate(blocks, 0).astype(jnp.bfloat16).astype(jnp.float32)
        squared_sum += jnp.where(diagonal, rounded, 0.0)
    part[0] = jnp.sum(kept_sum.reshape(LANE // 8, 8, LANE), 0)
    part[1] = jnp.sum(squared_sum.reshape(LANE // 8, 8, LANE), 0)

    for m in range(block_rows):
        at = pl.ds(m * BLK, BLK)
        squared[at, :] = (total_sum[at, :] * keep_filter[m : m + 1, :]).astype(jnp.bfloat16)

    def share(step_to, _):
        peer = lax.rem(me + step_to, row_size)
        pltpu.make_async_remote_copy(
            src_ref=part,
            dst_ref=parts.at[step_to],
            send_sem=tsend_sem.at[step_to],
            recv_sem=trecv_sem.at[step_to],
            device_id=(snap, peer, core),
            device_id_type=MESH,
        ).start()
        return 0

    lax.fori_loop(1, row_size, share, 0)

    for n in range(4):
        if n < 2:
            column = width + n * step
            place = (1 - core) * width + n * step
            deep = pl.ds(0, 3 * rows)
        else:
            column = 2 * core * width + (n - 2) * step
            place = core * width + (n - 2) * step
            deep = pl.ds(pl.multiple_of(core * rows, LANE), 2 * rows)
        at = pl.ds(pl.multiple_of(column, LANE), step)
        place = pl.ds(pl.multiple_of(place, LANE), step)
        tile = jnp.dot(
            squared[:, deep],
            right[deep, pl.ds(pl.multiple_of(width + column, LANE), step)],
            preferred_element_type=jnp.float32,
        )
        for m in range(block_rows):
            rows_at = pl.ds(m * BLK, BLK)
            result[rows_at, place] = 3.0 * squared[rows_at, at].astype(jnp.float32) - 2.0 * (
                tile[m * BLK : (m + 1) * BLK] * keep_filter[pl.ds(m, 1), at]
            )

    for m in range(block_rows):
        turn = (m * BLK) % LANE
        start = m * BLK - turn
        band = result[pl.ds(m * BLK, BLK), pl.ds(start, width + (LANE if turn else 0))]
        if turn:
            band = pltpu.roll(band, band.shape[1] - turn, 1)
        out[pl.ds(m * BLK, BLK), :] = band[:, :width].astype(jnp.bfloat16)

    def gather(step_to, sums):
        peer = lax.rem(me + row_size - step_to, row_size)
        pltpu.make_async_remote_copy(
            src_ref=part,
            dst_ref=parts.at[step_to],
            send_sem=tsend_sem.at[step_to],
            recv_sem=trecv_sem.at[step_to],
            device_id=(snap, peer, core),
            device_id_type=MESH,
        ).wait()
        return (sums[0] + parts[step_to, 0], sums[1] + parts[step_to, 1])

    sums = lax.fori_loop(1, row_size, gather, (part[0], part[1]))
    traces[0] = jnp.sum(sums[0]) / (total * BLK)
    traces[1] = jnp.sum(sums[1]) / (total * BLK)

    own.wait_send()
    for k in range(CHUNKS):
        to_partner(k).wait_send()
        across(p_side, core, k, send_sem.at[2, k], psib_sem.at[k]).wait_send()

        either(has_onward, lambda short: to_onward(k, short).wait_send())

        @pl.when(has_origin)
        def _():
            across(q_side, core, k, send_sem.at[3, k], qsib_sem.at[k]).wait_send()


def solution(mesh):
    row_size = mesh.shape["row"]

    def per_device(density, pattern, filter_mask):
        rows, width = density.shape
        block_rows = rows // BLK
        return pl.pallas_call(
            functools.partial(kernel, row_size),
            out_shape=(
                pltpu.VMEM((rows, width), jnp.bfloat16),
                jax.ShapeDtypeStruct((2,), jnp.float32),
            ),
            in_specs=[pl.BlockSpec(memory_space=pl.ANY)] * 3,
            out_specs=(
                pl.BlockSpec(memory_space=pltpu.VMEM),
                pl.BlockSpec(memory_space=pltpu.SMEM),
            ),
            scratch_shapes=[
                pltpu.VMEM((rows, width), jnp.bfloat16),
                pltpu.VMEM(pattern.shape, jnp.int32),
                pltpu.VMEM(filter_mask.shape, jnp.int32),
                pltpu.VMEM((2, rows, width), jnp.bfloat16),
                pltpu.VMEM((2, 2, rows, width), jnp.bfloat16),
                pltpu.VMEM((3 * rows, 5 * width), jnp.bfloat16),
                pltpu.VMEM((rows, 3 * width), jnp.float32),
                pltpu.VMEM((rows, 3 * width), jnp.bfloat16),
                pltpu.VMEM((block_rows, 3 * width), jnp.float32),
                pltpu.VMEM((rows, 2 * width), jnp.float32),
                pltpu.VMEM((2, 8, LANE), jnp.float32),
                pltpu.VMEM((row_size, 2, 8, LANE), jnp.float32),
                pltpu.SemaphoreType.DMA((5, CHUNKS)),
                pltpu.SemaphoreType.DMA,
                pltpu.SemaphoreType.DMA((CHUNKS,)),
                pltpu.SemaphoreType.DMA((CHUNKS,)),
                pltpu.SemaphoreType.DMA((CHUNKS,)),
                pltpu.SemaphoreType.DMA((CHUNKS,)),
                pltpu.SemaphoreType.DMA((row_size,)),
                pltpu.SemaphoreType.DMA((row_size,)),
                pltpu.SemaphoreType.DMA((3,)),
                pltpu.SemaphoreType.REGULAR((max(row_size // 2, 1),)),
                pltpu.SemaphoreType.REGULAR,
            ],
            compiler_params=pltpu.CompilerParams(
                collective_id=0, has_side_effects=True, vmem_limit_bytes=56 * 1024 * 1024
            ),
        )(density, pattern, filter_mask)

    return jax.shard_map(
        per_device,
        mesh=mesh,
        in_specs=(P(("snap", "row"), "col"), P(("snap", "row"), "col"), P(("snap", "row"), None)),
        out_specs=(P(("snap", "row"), "col"), P("snap")),
        check_vma=False,
    )
```
